32 devices in a mesh: dp: 8 (over y, x, core), head: 4 (over z).
Axes of the slice: x: 2, y: 2, z: 4, core: 2. Of those that a mesh axis runs over, the one named last changes fastest.
Arguments:
- feats: bfloat16 [4, 4096, 384], P('head', 'dp'), may hold values from -6 to 6
- valid: int32 [16], P('dp'), may hold values from 1 to 256
- owner_map: int32 [16], P('dp'), may hold values from 0 to 7, as said below
- w_conv: bfloat16 [4, 3, 384, 384], P('head', None, 'dp'), may hold values from -0.11785113 to 0.11785113
- w_mid: bfloat16 [4, 384, 384], P('head', 'dp'), may hold values from -0.20412415 to 0.20412415
- w_out: bfloat16 [4, 384], P('head', 'dp'), may hold values from -0.20412415 to 0.20412415
Outputs:
- grad_feats: bfloat16 [4, 8192, 384], P('head', 'dp')
- grad_conv: float32 [4, 3, 384, 384], P('head', None, 'dp')
- grad_mid: float32 [4, 384, 384], P('head', 'dp')
- grad_out: float32 [4, 384], P('head', 'dp')
The draws below stay inside these ranges and needn't reach their ends.
Inputs may be any that keep to these rules, and one draw needn't show every extreme that they name: `owner_map`: image o is held by index o of dp. Every image owns 1 to 4 blocks; a quarter of the images own exactly 4. The 2 blocks of one index of dp belong to 2 different images.
All inputs are finite; a program needn't handle non-finite values.
Results may differ from the reference program's by a relative error of at most 0.019.
Values may be sent and summed in bfloat16 or wider, within the bound.
A program may use at most 128 MiB of HBM per device.

```python
import jax
import jax.numpy as jnp
from jax import lax

D = 384
TAPS = 4
BT = 256
BLK_DEV = 2
CAP = 4
NB = 16
N_DP = 8


def draw_owner_map(key, part):
    devices = NB // BLK_DEV
    per_device = BLK_DEV
    first, second, third = jax.random.split(jax.random.fold_in(key, 7), 3)
    labels = jax.random.permutation(first, devices).astype(jnp.int32)
    position = jax.random.permutation(second, devices).astype(jnp.int32)
    member = jnp.where(position < devices // 2, 0, jnp.where(position < 3 * devices // 4, 1, jnp.where(position < 7 * devices // 8, 2, 3))).astype(jnp.int32)
    table = 4 * jnp.arange(per_device, dtype=jnp.int32)[None, :] + member[:, None]
    scores = jax.random.randint(third, (devices, per_device), 0, 1 << 20) * per_device + jnp.arange(per_device, dtype=jnp.int32)[None, :]
    order = jnp.argsort(scores, axis=1)
    table = jnp.take_along_axis(table, order, 1)
    return labels[table].reshape(-1).astype(jnp.int32)


def centered(values, spread, column_axis):
    values = values - jnp.mean(values, axis=column_axis, keepdims=True)
    return jnp.clip(values, -4.0 * spread, 4.0 * spread)


def draw_feats(key, part):
    first = jax.random.fold_in(jax.random.fold_in(key, 11), 0)
    shape = (TAPS, NB * BT, D)
    values = jax.random.normal(first, shape, jnp.float32)
    return jnp.clip(values, -6.0, 6.0).astype(jnp.bfloat16)


def draw_w_conv(key, part):
    first = jax.random.fold_in(key, 13)
    spread = (3.0 * D) ** (-0.5)
    shape = (TAPS, 3, D, D)
    values = jax.random.normal(first, shape, jnp.float32) * spread
    return jnp.clip(values, -4.0 * spread, 4.0 * spread).astype(jnp.bfloat16)


def draw_w_mid(key, part):
    first = jax.random.fold_in(key, 17)
    spread = D ** (-0.5)
    shape = (TAPS, D, D)
    values = jnp.clip(jax.random.normal(first, shape, jnp.float32), -4.0, 4.0) * spread
    return centered(values, spread, 1).astype(jnp.bfloat16)


def draw_w_out(key, part):
    first = jax.random.fold_in(key, 19)
    spread = D ** (-0.5)
    shape = (TAPS, D)
    values = jnp.clip(jax.random.normal(first, shape, jnp.float32), -4.0, 4.0) * spread
    return centered(values, spread, 1).astype(jnp.bfloat16)


def plant(drawn, key, smallest, top_value):
    spot = [jax.random.randint(jax.random.fold_in(key, axis), (), 0, length) for axis, length in enumerate(drawn.shape)]
    longest = drawn.shape.index(max(drawn.shape))
    beside = spot[:longest] + [(spot[longest] + 1) % drawn.shape[longest]] + spot[longest + 1:]
    return drawn.at[tuple(spot)].set(smallest).at[tuple(beside)].set(top_value)


def setup_inputs(seed: int = 0) -> dict:
    arg_keys = jax.random.split(jax.random.key(seed), 7)
    return {
        "feats": draw_feats(jax.random.fold_in(arg_keys[6], 71), 0),
        "valid": plant(jax.random.randint(arg_keys[1], (NB,), 1, BT + 1), jax.random.fold_in(arg_keys[1], 1), 1, BT).astype(jnp.int32),
        "owner_map": draw_owner_map(jax.random.fold_in(arg_keys[6], 71), 0),
        "w_conv": draw_w_conv(jax.random.fold_in(arg_keys[6], 71), 0),
        "w_mid": draw_w_mid(jax.random.fold_in(arg_keys[6], 71), 0),
        "w_out": draw_w_out(jax.random.fold_in(arg_keys[6], 71), 0),
    }


def activate(value):
    return 0.2 * value + 0.8 * jax.nn.softplus(value)

def derivative(value):
    return 0.2 + 0.8 * jax.nn.sigmoid(value)

def flatten(array):
    return array.reshape(-1, array.shape[-1])

def forward_pass(blocks, mask, conv_w, mid_w, out_w):
    count = blocks.shape[0]
    width = blocks.shape[2]
    masked = (blocks * mask[:, :, None]).astype(jnp.bfloat16)
    zero_row = jnp.zeros((count, 1, width), jnp.bfloat16)
    previous = jnp.concatenate([zero_row, masked[:, :-1]], 1)
    following = jnp.concatenate([masked[:, 1:], zero_row], 1)
    first_pre = jnp.dot(flatten(previous), conv_w[0], preferred_element_type=jnp.float32)
    first_pre = first_pre + jnp.dot(flatten(masked), conv_w[1], preferred_element_type=jnp.float32)
    first_pre = first_pre + jnp.dot(flatten(following), conv_w[2], preferred_element_type=jnp.float32)
    first_act = activate(first_pre)
    first_low = first_act.astype(jnp.bfloat16)
    second_pre = jnp.dot(first_low, mid_w, preferred_element_type=jnp.float32)
    second_act = activate(second_pre) + first_act
    logits = jnp.dot(second_act, out_w.astype(jnp.float32), precision=lax.Precision.HIGHEST)
    return ((previous, masked, following, first_pre, first_low, second_pre, second_act), logits)

def backward_pass(saved, upstream, mask, conv_w, mid_w, out_w):
    previous, masked, following, first_pre, first_low, second_pre, second_act = saved
    count, length, width = masked.shape
    grad_second = upstream[:, None] * out_w.astype(jnp.float32)[None, :]
    grad_mid_pre = (grad_second * derivative(second_pre)).astype(jnp.bfloat16)
    grad_first = jnp.dot(grad_mid_pre, mid_w.T, preferred_element_type=jnp.float32) + grad_second
    grad_first_pre = (grad_first * derivative(first_pre)).astype(jnp.bfloat16)

    def through(index):
        return jnp.dot(grad_first_pre, conv_w[index].T, preferred_element_type=jnp.float32).reshape(count, length, width)
    zero_row = jnp.zeros((count, 1, width), jnp.float32)
    from_next = through(0)
    from_prev = through(2)
    total = through(1) + jnp.concatenate([from_next[:, 1:], zero_row], 1) + jnp.concatenate([zero_row, from_prev[:, :-1]], 1)
    grad_input = (total * mask[:, :, None]).astype(jnp.bfloat16)
    grad_conv = jnp.stack([jnp.dot(flatten(previous).T, grad_first_pre, preferred_element_type=jnp.float32), jnp.dot(flatten(masked).T, grad_first_pre, preferred_element_type=jnp.float32), jnp.dot(flatten(following).T, grad_first_pre, preferred_element_type=jnp.float32)])
    grad_mid = jnp.dot(first_low.T, grad_mid_pre, preferred_element_type=jnp.float32)
    grad_out = jnp.dot(upstream, second_act, precision=lax.Precision.HIGHEST)
    return (grad_input, grad_conv, grad_mid, grad_out)

def reference(feats, valid, owner_map, w_conv, w_mid, w_out):
    blocks_all = owner_map.shape[0]
    member_int = (owner_map[:, None] == jnp.arange(N_DP, dtype=jnp.int32)[None, :]).astype(jnp.int32)
    earlier = jnp.cumsum(member_int, 0) - member_int
    slots = lax.optimization_barrier(jnp.sum(earlier * member_int, 1)).astype(jnp.int32)
    tokens = lax.optimization_barrier(jnp.sum(member_int * valid[:, None], 0)).astype(jnp.float32)
    members = member_int.astype(jnp.float32)
    mask = (jnp.arange(BT, dtype=jnp.int32)[None, :] < valid[:, None]).astype(jnp.float32)
    scale_norm = jnp.sqrt(TAPS * tokens)
    saved_all = []
    totals = jnp.zeros((N_DP,), jnp.float32)
    for tap in range(TAPS):
        blocks = feats[tap].reshape(blocks_all, BT, D)
        saved, logits = forward_pass(blocks, mask, w_conv[tap], w_mid[tap], w_out[tap])
        saved_all.append(saved)
        block_sums = lax.optimization_barrier(jnp.sum(logits.reshape(blocks_all, BT) * mask, 1))
        totals = totals + jnp.dot(block_sums, members, precision=lax.Precision.HIGHEST)
    strength = totals / scale_norm
    factor = -BT * jax.nn.sigmoid(-strength) / scale_norm
    upstream = (jnp.dot(members, factor, precision=lax.Precision.HIGHEST)[:, None] * mask).reshape(-1)
    target = (owner_map * CAP + slots).astype(jnp.int32)
    feat_list, conv_list, mid_list, out_list = ([], [], [], [])
    for tap in range(TAPS):
        grad_input, grad_conv, grad_mid, grad_out = backward_pass(saved_all[tap], upstream, mask, w_conv[tap], w_mid[tap], w_out[tap])
        placed = jnp.zeros((N_DP * CAP, BT, D), jnp.bfloat16).at[target].set(grad_input)
        feat_list.append(placed.reshape(N_DP * CAP * BT, D))
        conv_list.append(grad_conv / blocks_all)
        mid_list.append(grad_mid / blocks_all)
        out_list.append(grad_out / blocks_all)
    return (jnp.stack(feat_list), jnp.stack(conv_list), jnp.stack(mid_list), jnp.stack(out_list))
```

```python
import functools

import jax
import jax.numpy as jnp
from jax import lax
from jax.experimental import pallas as pl
from jax.experimental.pallas import tpu as pltpu
from jax.sharding import PartitionSpec as P

MESH = pl.DeviceIdType.MESH
F32 = jnp.float32
BF16 = jnp.bfloat16
LANES = 128


def dot(a, b, ca, cb):
    return lax.dot_general(a, b, (((ca,), (cb,)), ((), ())), preferred_element_type=F32)


def gates(z):
    t = jnp.exp(-jnp.abs(z))
    inv = 1.0 / (1.0 + t)
    act = 0.2 * z + 0.8 * (jnp.maximum(z, 0.0) + jnp.log(1.0 + t))
    der = 0.2 + 0.8 * jnp.where(z >= 0.0, inv, t * inv)
    return act, der


def kernel(
    n, heads, scale_taps,
    feats, valid, owner, wc, wm, wo,
    out, gco, gmo, goo,
    xcat, wbuf, wall, obuf, h1s, d1s, e2s, ecat, dxs, hsum,
    hbuf, mbuf, gbuf, sbuf, rbuf, part, psend, precv, qsend, qrecv,
    lsem, wsend, wrecv, osend, orecv, hsend, hrecv, msend, mrecv,
    gsend, grecv, dsend, drecv, psems, qs, qr,
):
    local, length, width = feats.shape
    rows = wm.shape[0]
    slots = out.shape[0]
    half = n // 2
    me = lax.axis_index("dp")
    hd = lax.axis_index("head")
    chip, core = lax.div(me, 2), lax.rem(me, 2)
    partner = me + 1 - 2 * core

    def dp(j):
        return {"dp": j}

    def ring(i):
        return lax.rem(me + i, n)

    def peer(i):
        return 2 * lax.rem(chip + i, half) + core

    def remote(src, dst, s, r, device):
        return pltpu.make_async_remote_copy(
            src_ref=src, dst_ref=dst, send_sem=s, recv_sem=r, device_id=device, device_id_type=MESH
        )

    barrier = pltpu.get_barrier_semaphore()
    for i in range(1, n):
        pl.semaphore_signal(barrier, inc=1, device_id=dp(ring(i)), device_id_type=MESH)
    for i in range(1, heads):
        pl.semaphore_signal(
            barrier, inc=1, device_id={"head": lax.rem(hd + i, heads)}, device_id_type=MESH
        )
    own_conv = pltpu.make_async_copy(wc, wbuf.at[me, pl.ds(0, 3)], lsem.at[0])
    own_mid = pltpu.make_async_copy(wm, wbuf.at[me, 3], lsem.at[1])
    own_conv.start()
    own_mid.start()
    pick = (
        lax.broadcasted_iota(jnp.int32, (rows, width), 1)
        == me * rows + lax.broadcasted_iota(jnp.int32, (rows, width), 0)
    ).astype(F32)
    obuf[me] = dot(
        jnp.broadcast_to(wo[...], (8, rows)), pick.astype(BF16), 1, 0
    )
    row = lax.broadcasted_iota(jnp.int32, (length, width), 0)
    pl.semaphore_wait(barrier, n - 1 + heads - 1)

    firsts = []
    for i in range(1, half):
        firsts.append((
            remote(wc, wbuf.at[me, pl.ds(0, 3)], wsend.at[i, 0], wrecv.at[i, 0], dp(peer(i))),
            remote(wm, wbuf.at[me, 3], wsend.at[i, 1], wrecv.at[i, 1], dp(peer(i))),
        ))
    near = (
        remote(wc, wbuf.at[me, pl.ds(0, 3)], wsend.at[0, 0], wrecv.at[0, 0], dp(partner)),
        remote(wm, wbuf.at[me, 3], wsend.at[0, 1], wrecv.at[0, 1], dp(partner)),
    )
    outs = [
        remote(obuf.at[me], obuf.at[me], osend.at[i], orecv.at[i], dp(ring(i))) for i in range(1, n)
    ]
    for copies in firsts:
        for copy in copies:
            copy.start()
    for copy in near:
        copy.start()
    for copy in outs:
        copy.start()

    def prepare(k, _):
        x = jnp.where(row < valid[k], feats[k].astype(F32), 0.0)
        xcat[k, 0] = jnp.where(row == 0, 0.0, pltpu.roll(x, 1, 0)).astype(BF16)
        xcat[k, 1] = x.astype(BF16)
        xcat[k, 2] = jnp.where(row == length - 1, 0.0, pltpu.roll(x, length - 1, 0)).astype(BF16)
        return 0

    lax.fori_loop(0, local, prepare, 0)

    relays = []
    for i, copies in enumerate(firsts, 1):
        for copy in copies:
            copy.wait_recv()
        j = 2 * lax.rem(chip - i + half, half) + core
        relay = remote(wbuf.at[j], wbuf.at[j], wsend.at[i, 2], wrecv.at[i, 2], dp(partner))
        relay.start()
        relays.append(relay)
    own_conv.wait()
    own_mid.wait()
    for copy in near:
        copy.wait_recv()
    for copy in outs:
        copy.wait_recv()
    for relay in relays:
        relay.wait_recv()
    for j in range(n):
        for s in range(4):
            wall[s, j * rows:(j + 1) * rows, :] = wbuf[j, s]
    w_out = obuf[0]
    for j in range(1, n):
        w_out = w_out + obuf[j]
    w_out = w_out[0:1]

    def forward(k, _):
        x = [xcat[k, s] for s in range(3)]
        z1 = dot(x[0], wall[0], 1, 0) + dot(x[1], wall[1], 1, 0) + dot(x[2], wall[2], 1, 0)
        a1, d1 = gates(z1)
        h1 = a1.astype(BF16)
        h1s[k] = h1
        d1s[k] = d1
        z2 = dot(h1, wall[3], 1, 0)
        a2, d2 = gates(z2)
        live = row < valid[k]
        hsum[k] = jnp.sum(jnp.where(live, a2 + a1, 0.0), 0, keepdims=True)
        e2s[k] = jnp.where(live, w_out * d2, 0.0).astype(BF16)
        return 0

    lax.fori_loop(0, local, forward, 0)

    padded = hbuf.shape[1]
    line = lax.broadcasted_iota(jnp.int32, (padded, LANES), 0)
    lane = lax.broadcasted_iota(jnp.int32, (padded, LANES), 1)
    sums = jnp.zeros((padded, LANES), F32)
    owners = jnp.full((padded, LANES), -1.0, F32)
    counts = jnp.zeros((padded, LANES), F32)
    for k in range(local):
        total = jnp.sum(hsum[k] * w_out, 1, keepdims=True)
        sums = jnp.where(line == k, total, sums)
        owners = jnp.where(line == k, owner[k].astype(F32), owners)
        counts = jnp.where(line == k, valid[k].astype(F32), counts)
    hbuf[hd] = sums
    hcopies = [
        remote(
            hbuf.at[hd], hbuf.at[hd], hsend.at[i], hrecv.at[i], {"head": lax.rem(hd + i, heads)}
        )
        for i in range(1, heads)
    ]
    for copy in hcopies:
        copy.start()

    def middle(k, _):
        live = row < valid[k]
        back = dot(e2s[k], wall[3], 1, 1) + jnp.where(live, w_out, 0.0)
        e1 = back * d1s[k]
        ecat[k, 0] = jnp.where(row == length - 1, 0.0, pltpu.roll(e1, length - 1, 0)).astype(BF16)
        ecat[k, 1] = e1.astype(BF16)
        ecat[k, 2] = jnp.where(row == 0, 0.0, pltpu.roll(e1, 1, 0)).astype(BF16)
        return 0

    lax.fori_loop(0, local, middle, 0)
    for copy in hcopies:
        copy.wait_recv()
    all_taps = hbuf[0]
    for t in range(1, heads):
        all_taps = all_taps + hbuf[t]
    mbuf[me] = jnp.where(lane == 0, owners, jnp.where(lane == 1, counts, all_taps))
    mcopies = [
        remote(mbuf.at[me], mbuf.at[me], msend.at[i], mrecv.at[i], dp(ring(i))) for i in range(1, n)
    ]
    for copy in mcopies:
        copy.start()

    def inward(k, _):
        total = (
            dot(ecat[k, 0], wall[0], 1, 1)
            + dot(ecat[k, 1], wall[1], 1, 1)
            + dot(ecat[k, 2], wall[2], 1, 1)
        )
        dxs[k] = jnp.where(row < valid[k], total, 0.0)
        return 0

    lax.fori_loop(0, local, inward, 0)
    for copy in mcopies:
        copy.wait_recv()
    meta = mbuf[...]
    holder = meta[:, :, 0:1]
    device = lax.broadcasted_iota(jnp.int32, (n, padded, 1), 0)
    factors = []
    for k in range(local):
        mine = jnp.where(holder == owner[k].astype(F32), meta, 0.0)
        mine = jnp.sum(jnp.sum(mine, 0), 0, keepdims=True)
        norm = jnp.sqrt(scale_taps * mine[:, 1:2])
        strength = mine[:, 2:3] / norm
        t = jnp.exp(-jnp.abs(strength))
        gate = jnp.where(strength >= 0.0, t, 1.0) / (1.0 + t)
        factors.append(-float(length) * gate / norm)

    dcopies = []
    for i in list(range(1, n)) + [0]:
        dst = ring(i)
        block = None
        for k in range(local):
            here = jnp.where(owner[k] == dst, 1.0, 0.0).astype(F32)
            term = dxs[k] * (factors[k] * here)
            block = term if block is None else block + term
        if i == 0:
            rbuf[0] = block.astype(BF16)
        else:
            sbuf[i] = block.astype(BF16)
            copy = remote(sbuf.at[i], rbuf.at[i], dsend.at[i], drecv.at[i], dp(dst))
            copy.start()
            dcopies.append(copy)

    go = None
    for k in range(local):
        term = hsum[k] * factors[k]
        go = term if go is None else go + term
    gbuf[me] = jnp.broadcast_to(go, (8, width))
    gcopies = [
        remote(gbuf.at[me], gbuf.at[me], gsend.at[i], grecv.at[i], dp(ring(i))) for i in range(1, n)
    ]
    for copy in gcopies:
        copy.start()

    def flat(ref, s=None):
        pieces = [ref[k] if s is None else ref[k, s] for k in range(local)]
        return jnp.concatenate(pieces, 0)

    def scaled(ref, s=None):
        pieces = [
            ((ref[k] if s is None else ref[k, s]).astype(F32) * factors[k]).astype(BF16)
            for k in range(local)
        ]
        return jnp.concatenate(pieces, 0)

    x_all = flat(xcat, 1)
    for s in range(4):
        if s < 3:
            grad = dot(x_all, scaled(ecat, s), 0, 0)
        else:
            grad = dot(flat(h1s), scaled(e2s), 0, 0)
        for j in range(n):
            part[j, s] = grad[j * rows:(j + 1) * rows, :]
    for q in range(half):
        psend[q] = part[2 * q + 1 - core].astype(BF16)
    pcopy = remote(psend, precv, psems.at[0], psems.at[1], dp(partner))
    pcopy.start()
    pcopy.wait_recv()
    qcopies = []
    for i in range(1, half):
        q = lax.rem(chip + i, half)
        qsend[i] = (part[2 * q + core] + precv[q].astype(F32)).astype(BF16)
        copy = remote(qsend.at[i], qrecv.at[i], qs.at[i], qr.at[i], dp(2 * q + core))
        copy.start()
        qcopies.append(copy)
    blocks = float(n * local)
    grads = part[me] + precv[chip].astype(F32)

    owned = jnp.where(holder == me.astype(F32), 1.0, 0.0)

    def weights(i):
        j = lax.rem(me - i + n, n)
        has = jnp.sum(jnp.sum(jnp.where(device == j, owned, 0.0), 0), 0, keepdims=True)
        slot = jnp.sum(jnp.sum(jnp.where(device < j, owned, 0.0), 0), 0, keepdims=True)
        return [jnp.where(slot == float(c), has, 0.0).astype(BF16) for c in range(slots)]

    w = weights(0)
    for c in range(slots):
        out[c] = rbuf[0] * w[c]
    for i in range(1, n):
        dcopies[i - 1].wait_recv()
        w = weights(i)
        for c in range(slots):
            out[c] = out[c] + rbuf[i] * w[c]

    for copy in gcopies:
        copy.wait_recv()
    go = gbuf[0]
    for j in range(1, n):
        go = go + gbuf[j]
    go = pltpu.roll(go * (1.0 / blocks), lax.rem(width - me * rows, width), 1)
    goo[...] = go[0:1, :rows]
    for i in range(1, half):
        qcopies[i - 1].wait_recv()
        grads = grads + qrecv[i].astype(F32)
    grads = grads / blocks
    gco[...] = grads[0:3]
    gmo[...] = grads[3]

    for copies in firsts + [near]:
        for copy in copies:
            copy.wait_send()
    for copy in relays + outs + hcopies + mcopies + dcopies + gcopies + qcopies + [pcopy]:
        copy.wait_send()


def solution(mesh):
    n, heads = mesh.shape["dp"], mesh.shape["head"]

    def per_device(feats, valid, owner_map, w_conv, w_mid, w_out):
        local = owner_map.shape[0]
        width = feats.shape[2]
        length = feats.shape[1] // local
        rows = w_mid.shape[1]
        slots = n // 2
        half = n // 2
        padded = -(-local // 8) * 8
        dma = pltpu.SemaphoreType.DMA
        vmem = pl.BlockSpec(memory_space=pltpu.VMEM)
        smem = pl.BlockSpec(memory_space=pltpu.SMEM)
        block = (local, length, width)
        scratch = [
            pltpu.VMEM((local, 3, length, width), BF16),
            pltpu.VMEM((n, 4, rows, width), BF16),
            pltpu.VMEM((4, width, width), BF16),
            pltpu.VMEM((n, 8, width), F32),
            pltpu.VMEM(block, BF16),
            pltpu.VMEM(block, F32),
            pltpu.VMEM(block, BF16),
            pltpu.VMEM((local, 3, length, width), BF16),
            pltpu.VMEM(block, F32),
            pltpu.VMEM((local, 1, width), F32),
            pltpu.VMEM((heads, padded, LANES), F32),
            pltpu.VMEM((n, padded, LANES), F32),
            pltpu.VMEM((n, 8, width), F32),
            pltpu.VMEM((n, length, width), BF16),
            pltpu.VMEM((n, length, width), BF16),
            pltpu.VMEM((n, 4, rows, width), F32),
            pltpu.VMEM((half, 4, rows, width), BF16),
            pltpu.VMEM((half, 4, rows, width), BF16),
            pltpu.VMEM((half, 4, rows, width), BF16),
            pltpu.VMEM((half, 4, rows, width), BF16),
            dma((2,)), dma((half, 3)), dma((half, 3)), dma((n,)), dma((n,)),
            dma((heads,)), dma((heads,)), dma((n,)), dma((n,)),
            dma((n,)), dma((n,)), dma((n,)), dma((n,)),
            dma((2,)), dma((half,)), dma((half,)),
        ]
        returned, conv, mid, last = pl.pallas_call(
            functools.partial(kernel, n, heads, float(heads)),
            out_shape=(
                jax.ShapeDtypeStruct((slots, length, width), BF16),
                jax.ShapeDtypeStruct((3, rows, width), F32),
                jax.ShapeDtypeStruct((rows, width), F32),
                jax.ShapeDtypeStruct((1, rows), F32),
            ),
            in_specs=[vmem, smem, smem, vmem, vmem, vmem],
            out_specs=(vmem, vmem, vmem, vmem),
            scratch_shapes=scratch,
            compiler_params=pltpu.CompilerParams(
                collective_id=0, has_side_effects=True, vmem_limit_bytes=60 * 1024 * 1024
            ),
        )(
            feats.reshape(block), valid, owner_map, w_conv[0], w_mid[0], w_out
        )
        return (
            returned.reshape(1, slots * length, width), conv[None], mid[None], last
        )

    in_specs = (
        P("head", "dp", None), P("dp"), P("dp"),
        P("head", None, "dp", None), P("head", "dp", None), P("head", "dp"),
    )
    out_specs = (
        P("head", "dp", None), P("head", None, "dp", None), P("head", "dp", None), P("head", "dp"),
    )
    return jax.shard_map(
        per_device, mesh=mesh, in_specs=in_specs, out_specs=out_specs, check_vma=False
    )
```

```python
import functools

import jax
import jax.numpy as jnp
from jax import lax
from jax.experimental import pallas as pl
from jax.experimental.pallas import tpu as pltpu
from jax.sharding import PartitionSpec as P

MESH = pl.DeviceIdType.MESH
F32 = jnp.float32
BF16 = jnp.bfloat16
LANES = 128


def dot(a, b, ca, cb):
    return lax.dot_general(a, b, (((ca,), (cb,)), ((), ())), preferred_element_type=F32)


def gates(z):
    t = jnp.exp(-jnp.abs(z))
    inv = 1.0 / (1.0 + t)
    act = 0.2 * z + 0.8 * (jnp.maximum(z, 0.0) + jnp.log(1.0 + t))
    der = 0.2 + 0.8 * jnp.where(z >= 0.0, inv, t * inv)
    return act, der


def kernel(
    n, heads, scale_taps,
    feats, valid, owner, wc, wm, wo,
    out, gco, gmo, goo,
    xcat, wbuf, wall, obuf, h1s, d1s, e2s, ecat, dxs, hsum,
    hbuf, mbuf, gbuf, sbuf, rbuf, part, psend, precv, qsend, qrecv,
    lsem, wsend, wrecv, osend, orecv, hsend, hrecv, msend, mrecv,
    gsend, grecv, dsend, drecv, psems, qs, qr,
):
    local, length, width = feats.shape
    rows = wm.shape[0]
    slots = out.shape[0]
    half = n // 2
    me = lax.axis_index("dp")
    hd = lax.axis_index("head")
    chip, core = lax.div(me, 2), lax.rem(me, 2)
    partner = me + 1 - 2 * core

    def dp(j):
        return {"dp": j}

    def ring(i):
        return lax.rem(me + i, n)

    def peer(i):
        return 2 * lax.rem(chip + i, half) + core

    def remote(src, dst, s, r, device):
        return pltpu.make_async_remote_copy(
            src_ref=src, dst_ref=dst, send_sem=s, recv_sem=r, device_id=device, device_id_type=MESH
        )

    barrier = pltpu.get_barrier_semaphore()
    for i in range(1, n):
        pl.semaphore_signal(barrier, inc=1, device_id=dp(ring(i)), device_id_type=MESH)
    for i in range(1, heads):
        pl.semaphore_signal(
            barrier, inc=1, device_id={"head": lax.rem(hd + i, heads)}, device_id_type=MESH
        )
    own_conv = pltpu.make_async_copy(wc, wbuf.at[me, pl.ds(0, 3)], lsem.at[0])
    own_mid = pltpu.make_async_copy(wm, wbuf.at[me, 3], lsem.at[1])
    own_conv.start()
    own_mid.start()
    pick = (
        lax.broadcasted_iota(jnp.int32, (rows, width), 1)
        == me * rows + lax.broadcasted_iota(jnp.int32, (rows, width), 0)
    ).astype(F32)
    obuf[me] = dot(
        jnp.broadcast_to(wo[...], (8, rows)), pick.astype(BF16), 1, 0
    )
    row = lax.broadcasted_iota(jnp.int32, (length, width), 0)
    pl.semaphore_wait(barrier, n - 1 + heads - 1)

    firsts = []
    for i in range(1, half):
        firsts.append((
            remote(wc, wbuf.at[me, pl.ds(0, 3)], wsend.at[i, 0], wrecv.at[i, 0], dp(peer(i))),
            remote(wm, wbuf.at[me, 3], wsend.at[i, 1], wrecv.at[i, 1], dp(peer(i))),
        ))
    near = (
        remote(wc, wbuf.at[me, pl.ds(0, 3)], wsend.at[0, 0], wrecv.at[0, 0], dp(partner)),
        remote(wm, wbuf.at[me, 3], wsend.at[0, 1], wrecv.at[0, 1], dp(partner)),
    )
    outs = [
        remote(obuf.at[me], obuf.at[me], osend.at[i], orecv.at[i], dp(ring(i))) for i in range(1, n)
    ]
    for copies in firsts:
        for copy in copies:
            copy.start()
    for copy in near:
        copy.start()
    for copy in outs:
        copy.start()

    def prepare(k, _):
        x = jnp.where(row < valid[k], feats[k].astype(F32), 0.0)
        xcat[k, 0] = jnp.where(row == 0, 0.0, pltpu.roll(x, 1, 0)).astype(BF16)
        xcat[k, 1] = x.astype(BF16)
        xcat[k, 2] = jnp.where(row == length - 1, 0.0, pltpu.roll(x, length - 1, 0)).astype(BF16)
        return 0

    lax.fori_loop(0, local, prepare, 0)

    relays = []
    for i, copies in enumerate(firsts, 1):
        for copy in copies:
            copy.wait_recv()
        j = 2 * lax.rem(chip - i + half, half) + core
        relay = remote(wbuf.at[j], wbuf.at[j], wsend.at[i, 2], wrecv.at[i, 2], dp(partner))
        relay.start()
        relays.append(relay)
    own_conv.wait()
    own_mid.wait()
    for copy in near:
        copy.wait_recv()
    for copy in outs:
        copy.wait_recv()
    for relay in relays:
        relay.wait_recv()
    for j in range(n):
        for s in range(4):
            wall[s, j * rows:(j + 1) * rows, :] = wbuf[j, s]
    w_out = obuf[0]
    for j in range(1, n):
        w_out = w_out + obuf[j]
    w_out = w_out[0:1]

    def forward(k, _):
        x = [xcat[k, s] for s in range(3)]
        z1 = dot(x[0], wall[0], 1, 0) + dot(x[1], wall[1], 1, 0) + dot(x[2], wall[2], 1, 0)
        a1, d1 = gates(z1)
        h1 = a1.astype(BF16)
        h1s[k] = h1
        d1s[k] = d1
        z2 = dot(h1, wall[3], 1, 0)
        a2, d2 = gates(z2)
        live = row < valid[k]
        hsum[k] = jnp.sum(jnp.where(live, a2 + a1, 0.0), 0, keepdims=True)
        e2s[k] = jnp.where(live, w_out * d2, 0.0).astype(BF16)
        return 0

    lax.fori_loop(0, local, forward, 0)

    padded = mbuf.shape[1]
    line = lax.broadcasted_iota(jnp.int32, (padded, LANES), 0)
    lane = lax.broadcasted_iota(jnp.int32, (padded, LANES), 1)
    sums = jnp.zeros((padded, LANES), F32)
    owners = jnp.full((padded, LANES), -1.0, F32)
    counts = jnp.zeros((padded, LANES), F32)
    for k in range(local):
        total = jnp.sum(hsum[k] * w_out, 1, keepdims=True)
        sums = jnp.where(line == k, total, sums)
        owners = jnp.where(line == k, owner[k].astype(F32), owners)
        counts = jnp.where(line == k, valid[k].astype(F32), counts)
    mbuf[me] = jnp.where(lane == 0, owners, jnp.where(lane == 1, counts, sums))
    mcopies = [
        remote(mbuf.at[me], mbuf.at[me], msend.at[i], mrecv.at[i], dp(ring(i))) for i in range(1, n)
    ]
    for copy in mcopies:
        copy.start()

    def middle(k, _):
        live = row < valid[k]
        back = dot(e2s[k], wall[3], 1, 1) + jnp.where(live, w_out, 0.0)
        e1 = back * d1s[k]
        ecat[k, 0] = jnp.where(row == length - 1, 0.0, pltpu.roll(e1, length - 1, 0)).astype(BF16)
        ecat[k, 1] = e1.astype(BF16)
        ecat[k, 2] = jnp.where(row == 0, 0.0, pltpu.roll(e1, 1, 0)).astype(BF16)
        return 0

    lax.fori_loop(0, local, middle, 0)
    def inward(k, _):
        total = (
            dot(ecat[k, 0], wall[0], 1, 1)
            + dot(ecat[k, 1], wall[1], 1, 1)
            + dot(ecat[k, 2], wall[2], 1, 1)
        )
        dxs[k] = jnp.where(row < valid[k], total, 0.0)
        return 0

    lax.fori_loop(0, local, inward, 0)
    for copy in mcopies:
        copy.wait_recv()
    hbuf[hd] = mbuf[...]
    hcopies = [
        remote(
            hbuf.at[hd], hbuf.at[hd], hsend.at[i], hrecv.at[i], {"head": lax.rem(hd + i, heads)}
        )
        for i in range(1, heads)
    ]
    for copy in hcopies:
        copy.start()

    dcopies = []
    for i in list(range(1, n)) + [0]:
        dst = ring(i)
        block = None
        for k in range(local):
            here = jnp.where(owner[k] == dst, 1.0, 0.0).astype(F32)
            term = dxs[k] * here
            block = term if block is None else block + term
        if i == 0:
            rbuf[0] = block.astype(BF16)
        else:
            sbuf[i] = block.astype(BF16)
            copy = remote(sbuf.at[i], rbuf.at[i], dsend.at[i], drecv.at[i], dp(dst))
            copy.start()
            dcopies.append(copy)

    for copy in hcopies:
        copy.wait_recv()
    meta = hbuf[0]
    spread = lax.broadcasted_iota(jnp.int32, meta.shape, 2)
    for t in range(1, heads):
        meta = jnp.where(spread < 2, meta, meta + hbuf[t])
    holder = meta[:, :, 0:1]
    device = lax.broadcasted_iota(jnp.int32, (n, padded, 1), 0)

    def factor_of(image):
        mine = jnp.where(holder == image.astype(F32), meta, 0.0)
        mine = jnp.sum(jnp.sum(mine, 0), 0, keepdims=True)
        norm = jnp.sqrt(scale_taps * jnp.maximum(mine[:, 1:2], 1.0))
        strength = mine[:, 2:3] / norm
        t = jnp.exp(-jnp.abs(strength))
        gate = jnp.where(strength >= 0.0, t, 1.0) / (1.0 + t)
        return -float(length) * gate / norm

    factors = [factor_of(owner[k]) for k in range(local)]
    mine = factor_of(me)

    go = None
    for k in range(local):
        term = hsum[k] * factors[k]
        go = term if go is None else go + term
    gbuf[me] = jnp.broadcast_to(go, (8, width))
    gcopies = [
        remote(gbuf.at[me], gbuf.at[me], gsend.at[i], grecv.at[i], dp(ring(i))) for i in range(1, n)
    ]
    for copy in gcopies:
        copy.start()

    def flat(ref, s=None):
        pieces = [ref[k] if s is None else ref[k, s] for k in range(local)]
        return jnp.concatenate(pieces, 0)

    def scaled(ref, s=None):
        pieces = [
            ((ref[k] if s is None else ref[k, s]).astype(F32) * factors[k]).astype(BF16)
            for k in range(local)
        ]
        return jnp.concatenate(pieces, 0)

    x_all = flat(xcat, 1)
    for s in range(4):
        if s < 3:
            grad = dot(x_all, scaled(ecat, s), 0, 0)
        else:
            grad = dot(flat(h1s), scaled(e2s), 0, 0)
        for j in range(n):
            part[j, s] = grad[j * rows:(j + 1) * rows, :]
    for q in range(half):
        psend[q] = part[2 * q + 1 - core].astype(BF16)
    pcopy = remote(psend, precv, psems.at[0], psems.at[1], dp(partner))
    pcopy.start()
    pcopy.wait_recv()
    qcopies = []
    for i in range(1, half):
        q = lax.rem(chip + i, half)
        qsend[i] = (part[2 * q + core] + precv[q].astype(F32)).astype(BF16)
        copy = remote(qsend.at[i], qrecv.at[i], qs.at[i], qr.at[i], dp(2 * q + core))
        copy.start()
        qcopies.append(copy)
    blocks = float(n * local)
    grads = part[me] + precv[chip].astype(F32)

    owned = jnp.where(holder == me.astype(F32), 1.0, 0.0)

    def weights(i):
        j = lax.rem(me - i + n, n)
        has = jnp.sum(jnp.sum(jnp.where(device == j, owned, 0.0), 0), 0, keepdims=True)
        slot = jnp.sum(jnp.sum(jnp.where(device < j, owned, 0.0), 0), 0, keepdims=True)
        return [jnp.where(slot == float(c), has * mine, 0.0) for c in range(slots)]

    w = weights(0)
    for c in range(slots):
        out[c] = (rbuf[0].astype(F32) * w[c]).astype(BF16)
    for i in range(1, n):
        dcopies[i - 1].wait_recv()
        w = weights(i)
        for c in range(slots):
            out[c] = out[c] + (rbuf[i].astype(F32) * w[c]).astype(BF16)

    for copy in gcopies:
        copy.wait_recv()
    go = gbuf[0]
    for j in range(1, n):
        go = go + gbuf[j]
    go = pltpu.roll(go * (1.0 / blocks), lax.rem(width - me * rows, width), 1)
    goo[...] = go[0:1, :rows]
    for i in range(1, half):
        qcopies[i - 1].wait_recv()
        grads = grads + qrecv[i].astype(F32)
    grads = grads / blocks
    gco[...] = grads[0:3]
    gmo[...] = grads[3]

    for copies in firsts + [near]:
        for copy in copies:
            copy.wait_send()
    for copy in relays + outs + hcopies + mcopies + dcopies + gcopies + qcopies + [pcopy]:
        copy.wait_send()


def solution(mesh):
    n, heads = mesh.shape["dp"], mesh.shape["head"]

    def per_device(feats, valid, owner_map, w_conv, w_mid, w_out):
        local = owner_map.shape[0]
        width = feats.shape[2]
        length = feats.shape[1] // local
        rows = w_mid.shape[1]
        slots = n // 2
        half = n // 2
        padded = -(-local // 8) * 8
        dma = pltpu.SemaphoreType.DMA
        vmem = pl.BlockSpec(memory_space=pltpu.VMEM)
        smem = pl.BlockSpec(memory_space=pltpu.SMEM)
        block = (local, length, width)
        scratch = [
            pltpu.VMEM((local, 3, length, width), BF16),
            pltpu.VMEM((n, 4, rows, width), BF16),
            pltpu.VMEM((4, width, width), BF16),
            pltpu.VMEM((n, 8, width), F32),
            pltpu.VMEM(block, BF16),
            pltpu.VMEM(block, F32),
            pltpu.VMEM(block, BF16),
            pltpu.VMEM((local, 3, length, width), BF16),
            pltpu.VMEM(block, F32),
            pltpu.VMEM((local, 1, width), F32),
            pltpu.VMEM((heads, n, padded, LANES), F32),
            pltpu.VMEM((n, padded, LANES), F32),
            pltpu.VMEM((n, 8, width), F32),
            pltpu.VMEM((n, length, width), BF16),
            pltpu.VMEM((n, length, width), BF16),
            pltpu.VMEM((n, 4, rows, width), F32),
            pltpu.VMEM((half, 4, rows, width), BF16),
            pltpu.VMEM((half, 4, rows, width), BF16),
            pltpu.VMEM((half, 4, rows, width), BF16),
            pltpu.VMEM((half, 4, rows, width), BF16),
            dma((2,)), dma((half, 3)), dma((half, 3)), dma((n,)), dma((n,)),
            dma((heads,)), dma((heads,)), dma((n,)), dma((n,)),
            dma((n,)), dma((n,)), dma((n,)), dma((n,)),
            dma((2,)), dma((half,)), dma((half,)),
        ]
        returned, conv, mid, last = pl.pallas_call(
            functools.partial(kernel, n, heads, float(heads)),
            out_shape=(
                jax.ShapeDtypeStruct((slots, length, width), BF16),
                jax.ShapeDtypeStruct((3, rows, width), F32),
                jax.ShapeDtypeStruct((rows, width), F32),
                jax.ShapeDtypeStruct((1, rows), F32),
            ),
            in_specs=[vmem, smem, smem, vmem, vmem, vmem],
            out_specs=(vmem, vmem, vmem, vmem),
            scratch_shapes=scratch,
            compiler_params=pltpu.CompilerParams(
                collective_id=0, has_side_effects=True, vmem_limit_bytes=60 * 1024 * 1024
            ),
        )(
            feats.reshape(block), valid, owner_map, w_conv[0], w_mid[0], w_out
        )
        return (
            returned.reshape(1, slots * length, width), conv[None], mid[None], last
        )

    in_specs = (
        P("head", "dp", None), P("dp"), P("dp"),
        P("head", None, "dp", None), P("head", "dp", None), P("head", "dp"),
    )
    out_specs = (
        P("head", "dp", None), P("head", None, "dp", None), P("head", "dp", None), P("head", "dp"),
    )
    return jax.shard_map(
        per_device, mesh=mesh, in_specs=in_specs, out_specs=out_specs, check_vma=False
    )
```
